32 devices in a mesh: bx: 8 (over y, x, core), by: 4 (over z).
Axes of the slice: x: 2, y: 2, z: 4, core: 2. Of those that a mesh axis runs over, the one named last changes fastest.
Arguments:
- photon_data: float32 [6, 512, 128, 128], P(None, 'bx', 'by'), may hold values from 0 to 1, as said below
- block_counts: int32 [512, 128], P('bx', 'by'), may hold values from 1 to 128
- gather_offsets: float32 [3, 131072], P(None, ('bx', 'by')), may hold values from 0 to 1, as said below
- gather_blocks: int32 [4, 131072], P(None, ('bx', 'by')), may hold values from 0 to 65535, as said below
- albedo: float32 [3, 131072], P(None, ('bx', 'by')), may hold values from 0.1 to 1
- gather_pixels: int32 [131072], P(('bx', 'by')), may hold values from 0 to 65535, as said below
- tile_slot: int32 [256], replicated, may hold values from 0 to 255, as said below
Outputs:
- film: float32 [3, 256, 256], P(None, ('bx', 'by'))
The draws below stay inside these ranges and needn't reach their ends.
Inputs may be any that keep to these rules, and one draw needn't show every extreme that they name: `photon_data`: per point and channel in cell units: entries 0 to 2 are a position in [0, 1), entries 3 to 5 a positive power. `gather_offsets`: each coordinate lies in [0, 1). `gather_blocks`: entry 0 is the point's own cell, inside the brick of the device that holds the point; the 4 entries are the four different cells of a 2 x 2 square of cells (periodic) that contains it. `gather_pixels`: in the rows of one device, at most 384 gather points lie in tiles whose slots s share s // 8; in every draw some such owner group receives exactly 384 from every device. `tile_slot`: A permutation of 0 to 255.
All inputs are finite; a program needn't handle non-finite values.
Results may differ from the reference program's by a relative error of at most 0.0003.
Values sent between devices are 32-bit elements; how exact they have to be, the bound alone decides.
A program may use at most 512 MiB of HBM per device.

```python
import math
import jax
import jax.numpy as jnp
from jax import lax

CX = 64
CY = 32
SLOTS = 128
LISTED = 4
G_DEV = 4096
TILE_PIX = 256
TILE_DEV = 8
OWNERS = 32
NXC = 512
NYC = 128
NG = 131072
TILES = 256
CAP = 384


def gather_geometry(key):
    base = jax.random.fold_in(key, 11)
    keys = jax.random.split(base, 5)
    rows = jnp.arange(NG, dtype=jnp.int32)
    device = rows // G_DEV
    bricks_y = NYC // CY
    home_x = device // bricks_y * CX + jax.random.randint(keys[0], (NG,), 0, CX)
    home_y = device % bricks_y * CY + jax.random.randint(keys[1], (NG,), 0, CY)
    step_x = 2 * jax.random.randint(keys[2], (NG,), 0, 2) - 1
    step_y = 2 * jax.random.randint(keys[3], (NG,), 0, 2) - 1
    turn = jax.random.randint(keys[4], (NG,), 0, 3)
    return (home_x, home_y, step_x, step_y, turn)


def owner_plan(key):
    base = jax.random.fold_in(key, 23)
    keys = jax.random.split(base, 5)
    perm = jax.random.permutation(keys[0], TILES).astype(jnp.int32)
    pool = OWNERS * CAP
    heavy = jax.random.randint(keys[1], (), 0, OWNERS)
    owner_of = jnp.arange(pool, dtype=jnp.int32) // CAP

    def one_device(dev_key):
        scores = jax.random.permutation(dev_key, pool).astype(jnp.int32)
        order = jnp.argsort(jnp.where(owner_of == heavy, 0, pool) + scores, stable=True)
        picked = order[:G_DEV] // CAP
        mixing = jax.random.permutation(jax.random.fold_in(dev_key, 1), G_DEV)
        return picked[mixing].astype(jnp.int32)
    dev_keys = jax.vmap(lambda d: jax.random.fold_in(keys[2], d))(jnp.arange(OWNERS))
    owner = jax.vmap(one_device)(dev_keys).reshape(NG)
    local_tile = jax.random.randint(keys[3], (NG,), 0, TILE_DEV)
    slot = owner * TILE_DEV + local_tile
    inverse = jnp.argsort(perm, stable=True).astype(jnp.int32)
    tile = inverse[slot]
    pixel = tile * TILE_PIX + jax.random.randint(keys[4], (NG,), 0, TILE_PIX)
    return (perm, pixel.astype(jnp.int32))


def draw_tile_slot(key, part):
    return owner_plan(key)[0]


def draw_gather_pixels(key, part):
    return owner_plan(key)[1]


def draw_gather_blocks(key, part):
    home_x, home_y, step_x, step_y, turn = gather_geometry(key)
    own = home_x * NYC + home_y
    beside_x = (home_x + step_x) % NXC * NYC + home_y
    beside_y = home_x * NYC + (home_y + step_y) % NYC
    beside_xy = (home_x + step_x) % NXC * NYC + (home_y + step_y) % NYC
    others = jnp.stack([beside_x, beside_y, beside_xy])
    picks = []
    for entry in range(3):
        which = (entry + turn) % 3
        picks.append(jnp.where(which == 0, others[0], jnp.where(which == 1, others[1], others[2])))
    return jnp.stack([own] + picks).astype(jnp.int32)


def draw_gather_offsets(key, part):
    home_x, home_y, step_x, step_y, turn = gather_geometry(key)
    uniforms = jax.random.uniform(jax.random.fold_in(key, 12), (3, NG), jnp.float32, 0.0, 0.999)
    off_x = jnp.where(step_x > 0, 0.5 + 0.49 * uniforms[0], 0.5 - 0.5 * uniforms[0])
    off_y = jnp.where(step_y > 0, 0.5 + 0.49 * uniforms[1], 0.5 - 0.5 * uniforms[1])
    return jnp.stack([off_x, off_y, uniforms[2]]).astype(jnp.float32)


def draw_photon_data(key, part):
    keys = jax.random.split(jax.random.fold_in(key, 31), 2)
    places = jax.random.uniform(keys[0], (3, NXC, NYC, SLOTS), jnp.float32, 0.0, 0.999)
    log_power = jax.random.uniform(keys[1], (3, NXC, NYC, SLOTS), jnp.float32, jnp.log(0.02), jnp.log(0.2))
    power = jnp.exp(log_power)
    return jnp.concatenate([places, power], axis=0).astype(jnp.float32)


def place_ends(result, rng, smallest, largest):
    longest = result.shape.index(max(result.shape))
    spots = []
    for shift in (0, 1):
        where = [jax.random.randint(jax.random.fold_in(rng, axis), (), 0, length) for axis, length in enumerate(result.shape)]
        where[longest] = (where[longest] + shift) % result.shape[longest]
        spots.append(tuple(where))
    return result.at[spots[0]].set(smallest).at[spots[1]].set(largest)


def block_scale(own_key, dims, cuts, low, largest):
    factor_of, own = 1.0, jax.random.fold_in(own_key, 6)
    for position, blocks in cuts:
        draws = jnp.exp(jax.random.uniform(jax.random.fold_in(own, position), (blocks,), jnp.float32, low / len(cuts), largest / len(cuts)))
        factor_of = factor_of * jnp.repeat(draws, dims[position] // blocks).reshape([-1 if axis == position else 1 for axis in range(len(dims))])
    return factor_of


def setup_inputs(seed: int = 0) -> dict:
    splits = jax.random.split(jax.random.key(seed), 8)
    return {
        "photon_data": draw_photon_data(jax.random.fold_in(splits[7], 71), 0),
        "block_counts": place_ends(jax.random.randint(splits[1], (NXC, NYC), 1, SLOTS + 1), jax.random.fold_in(splits[1], 1), 1, SLOTS).astype(jnp.int32),
        "gather_offsets": draw_gather_offsets(jax.random.fold_in(splits[7], 71), 0),
        "gather_blocks": draw_gather_blocks(jax.random.fold_in(splits[7], 71), 0),
        "albedo": jnp.clip(jnp.exp(math.log(1.0) - 2.3025851 * jax.random.uniform(splits[4], (3, NG), jnp.float32) ** block_scale(splits[4], (3, NG), ((1, 32),), -0.2, 0.2)), 0.1, 1.0),
        "gather_pixels": draw_gather_pixels(jax.random.fold_in(splits[7], 71), 0),
        "tile_slot": draw_tile_slot(jax.random.fold_in(splits[7], 71), 0),
    }


RADIUS_SQ = 0.25


def kernel_sum(blocks, live, shift_x, shift_y, offsets, albedo):
    delta_x = (shift_x[:, :, None] + blocks[0]) - offsets[0][:, None, None]
    delta_y = (shift_y[:, :, None] + blocks[1]) - offsets[1][:, None, None]
    delta_z = blocks[2] - offsets[2][:, None, None]
    dist_sq = delta_x * delta_x + delta_y * delta_y + delta_z * delta_z
    weight = jnp.maximum(1.0 - dist_sq / RADIUS_SQ, 0.0)
    weight = jnp.where(live, weight, 0.0)
    sums = jnp.sum(weight[None] * blocks[3:6], axis=(2, 3))
    return albedo * sums


def reference(photon_data, block_counts, gather_offsets, gather_blocks, albedo, gather_pixels, tile_slot):
    slots = photon_data.shape[3]
    table = photon_data.reshape(6, NXC * NYC, slots)
    count_table = block_counts.reshape(NXC * NYC)
    group = math.gcd(NG, 4096)
    groups = NG // group
    ids = gather_blocks.reshape(LISTED, groups, group).transpose(1, 2, 0)
    offs = gather_offsets.reshape(3, groups, group).transpose(1, 0, 2)
    albs = albedo.reshape(3, groups, group).transpose(1, 0, 2)

    def one_group(packed):
        idb, off, alb = packed
        cell_x = idb // NYC
        cell_y = idb % NYC
        shift_x = ((cell_x - cell_x[:, :1] + 1) % NXC - 1).astype(jnp.float32)
        shift_y = ((cell_y - cell_y[:, :1] + 1) % NYC - 1).astype(jnp.float32)
        flat = idb.reshape(-1)
        blocks = jnp.take(table, flat, axis=1).reshape(6, group, LISTED, slots)
        counts = jnp.take(count_table, flat).reshape(group, LISTED)
        live = jnp.arange(slots, dtype=jnp.int32)[None, None, :] < counts[:, :, None]
        return kernel_sum(blocks, live, shift_x, shift_y, off, alb)

    rad = lax.map(one_group, (ids, offs, albs))
    radiance = rad.transpose(1, 0, 2).reshape(3, NG)
    tile = gather_pixels // TILE_PIX
    slot = jnp.take(tile_slot, tile)
    target = slot * TILE_PIX + gather_pixels % TILE_PIX
    film = jnp.zeros((3, TILES * TILE_PIX), jnp.float32).at[:, target].add(radiance)
    return film.reshape(3, TILES, TILE_PIX)
```

```python
import functools

import jax
import jax.numpy as jnp
from jax import lax
from jax.experimental import pallas as pl
from jax.experimental.pallas import tpu as pltpu
from jax.sharding import PartitionSpec as P

TILE_PIX = 256
INV_RADIUS_SQ = 4.0
FAR = 1.0e4
LANES = 128
ROWS = 8
CHANNELS = 6
MESH = pl.DeviceIdType.MESH
NT = (((1,), (1,)), ((), ()))
PITCH = 9
GROUP = 4 * ROWS * PITCH
SQUARE = ((0, 0), (0, 1), (1, 0), (1, 1))


def split_by(value, size):
    if size & (size - 1) == 0:
        return value >> (size.bit_length() - 1), value & (size - 1)
    return lax.div(value, size), lax.rem(value, size)


def whole_kernel(
    nx, ny, cap_rows, tiles_dev,
    photons, counts, offsets, blocks, albedo, pixels, tile_slot, out,
    table, edge_x, edge_y, stage_a, stage_b, wide_a, wide_b, acc_a, acc_b,
    spread, tri, count_row, count_col, points_v, base_v, base_s, owner_v, pixel_v,
    packed, send, recv,
    fill_sem, edge_sem, base_sem, halo_send, halo_recv, send_sem, recv_sem,
):
    cx, cy = photons.shape[1], photons.shape[2]
    pitch_y = cy + 2
    grid_x, grid_y = cx * nx, cy * ny
    points = offsets.shape[1]
    steps = points // LANES
    owners = nx * ny
    pitch = send.shape[1]
    used = 4 * cap_rows
    ix, iy = lax.axis_index("bx"), lax.axis_index("by")
    me = ix * ny + iy

    edges = []
    for c in range(CHANNELS):
        for s, x in enumerate((cx - 1, 0)):
            edges.append(
                pltpu.make_async_copy(
                    photons.at[c, x], edge_x.at[s, :, c], edge_sem.at[len(edges)]
                )
            )
        for s, y in enumerate((cy - 1, 0)):
            edges.append(
                pltpu.make_async_copy(
                    photons.at[c, :, y], edge_y.at[s, :, c], edge_sem.at[len(edges)]
                )
            )
    for edge in edges:
        edge.start()
    fills = [
        pltpu.make_async_copy(
            photons.at[c], table.at[pl.ds(1, cx), pl.ds(1, cy), c], fill_sem.at[c]
        )
        for c in range(CHANNELS)
    ]
    for fill in fills:
        fill.start()
    barrier = pltpu.get_barrier_semaphore()

    def greet(s, _):
        to = lax.rem(me + s, owners)
        pl.semaphore_signal(
            barrier, inc=1, device_id=(to // ny, lax.rem(to, ny)), device_id_type=MESH
        )
        return 0

    lax.fori_loop(1, owners, greet, 0)

    count_row[...] = counts[...].astype(jnp.float32)
    square = jnp.concatenate(
        [count_row[...], jnp.zeros((cy, LANES - cx), jnp.float32)], axis=1
    )
    square = jnp.concatenate([square, jnp.zeros((LANES - cy, LANES), jnp.float32)], axis=0)
    count_col[...] = square.T
    lane = lax.broadcasted_iota(jnp.int32, (ROWS, LANES), 1).astype(jnp.float32)

    def hide(ref, first, column):
        rows = column.shape[0]
        for r in range(0, rows, ROWS):
            place = pl.ds(first + r * ROWS, ROWS, stride=ROWS)
            ref[place, :] = jnp.where(lane < column[r : r + ROWS], ref[place, :], FAR)

    for edge in edges:
        edge.wait()
    flat_x = edge_x.reshape(2 * cy * ROWS, LANES)
    flat_y = edge_y.reshape(2 * cx * ROWS, LANES)
    for s, x in enumerate((cx - 1, 0)):
        hide(flat_x, s * cy * ROWS, count_row[:, x : x + 1])
    for s, y in enumerate((cy - 1, 0)):
        hide(flat_y, s * cx * ROWS, count_col[0:cx, y : y + 1])
    pl.semaphore_wait(barrier, owners - 1)

    right, left = lax.rem(ix + 1, nx), lax.rem(ix + nx - 1, nx)
    up, down = lax.rem(iy + 1, ny), lax.rem(iy + ny - 1, ny)
    data = pl.ds(0, CHANNELS)
    wide_x, wide_y = pl.ds(1, cx), pl.ds(1, cy)
    parts = [
        (edge_y.at[0, :, data], table.at[wide_x, 0, data], ix, up),
        (edge_y.at[1, :, data], table.at[wide_x, cy + 1, data], ix, down),
        (edge_x.at[0, :, data], table.at[0, wide_y, data], right, iy),
        (edge_x.at[1, :, data], table.at[cx + 1, wide_y, data], left, iy),
        (edge_x.at[0, cy - 1, data], table.at[0, 0, data], right, up),
        (edge_x.at[0, 0, data], table.at[0, cy + 1, data], right, down),
        (edge_x.at[1, cy - 1, data], table.at[cx + 1, 0, data], left, up),
        (edge_x.at[1, 0, data], table.at[cx + 1, cy + 1, data], left, down),
    ]
    halos = [
        pltpu.make_async_remote_copy(
            src_ref=src, dst_ref=dst, send_sem=halo_send.at[n], recv_sem=halo_recv.at[n],
            device_id=(px, py), device_id_type=MESH,
        )
        for n, (src, dst, px, py) in enumerate(parts)
    ]
    for halo in halos:
        halo.start()

    cell_x, cell_y = split_by(blocks[...], grid_y)

    def local(cell, first, size):
        t = cell - first + 1
        t = jnp.where(t < 0, t + size, t)
        return jnp.where(t >= size, t - size, t)

    lx, ly = local(cell_x, ix * cx, grid_x), local(cell_y, iy * cy, grid_y)
    low_x, low_y = jnp.min(lx, axis=0, keepdims=True), jnp.min(ly, axis=0, keepdims=True)
    base = jnp.minimum(low_x, cx) * pitch_y + jnp.minimum(low_y, cy)
    for j in range(steps):
        base_v[j : j + 1, :] = base[:, j * LANES : (j + 1) * LANES]
    to_scalar = pltpu.make_async_copy(base_v, base_s, base_sem)
    to_scalar.start()
    points_v[...] = jnp.zeros_like(points_v)
    points_v[0:1, :] = offsets[0:1, :] + (lx[0:1] - low_x).astype(jnp.float32)
    points_v[1:2, :] = offsets[1:2, :] + (ly[0:1] - low_y).astype(jnp.float32)
    points_v[2:3, :] = offsets[2:3, :]

    tile, within = split_by(pixels[...], TILE_PIX)

    def look_up(t, found):
        for u in range(ROWS):
            n = t * ROWS + u
            found = jnp.where(tile == n, tile_slot[n], found)
        return found

    slot = lax.fori_loop(0, tile_slot.shape[0] // ROWS, look_up, jnp.zeros_like(tile))
    owner, place = split_by(slot, tiles_dev)
    half, low = split_by(within, LANES)
    owner_v[...] = jnp.full(owner_v.shape, -1, jnp.int32)
    owner_v[pl.ds(ROWS, steps), :] = owner
    pixel_v[0:steps, :] = half * tiles_dev + place
    pixel_v[steps : 2 * steps, :] = low

    a = lax.broadcasted_iota(jnp.int32, (LANES, LANES), 0)
    b = lax.broadcasted_iota(jnp.int32, (LANES, LANES), 1)
    tri[...] = jnp.where(a < b, 1.0, 0.0).astype(jnp.bfloat16)
    a = lax.broadcasted_iota(jnp.int32, spread.shape, 0)
    b = lax.broadcasted_iota(jnp.int32, spread.shape, 1)
    spread[...] = jnp.where(a % ROWS == b // LANES, 1.0, 0.0).astype(jnp.bfloat16)
    packed[...] = jnp.zeros_like(packed)
    acc_b[...] = jnp.zeros_like(acc_b)

    for fill in fills:
        fill.wait()
    flat = table.reshape((cx + 2) * pitch_y * ROWS, LANES)
    cells = table.reshape((cx + 2) * pitch_y, ROWS, LANES)
    for x in range(cx):
        hide(flat, ((x + 1) * pitch_y + 1) * ROWS, count_row[:, x : x + 1])
    to_scalar.wait()
    for halo in halos:
        halo.wait()

    own_iota = lax.broadcasted_iota(jnp.int32, (owners, LANES), 0)
    cap_iota = lax.broadcasted_iota(jnp.int32, (cap_rows * LANES, LANES), 0).astype(jnp.float32)

    def widen(step, wide):
        value = points_v[:, pl.ds(pl.multiple_of(step * LANES, LANES), LANES)]
        pieces = []
        for _ in range(3):
            high = value.astype(jnp.bfloat16)
            pieces.append(high)
            value = value - high.astype(jnp.float32)
        wide[...] = lax.dot_general(
            jnp.concatenate(pieces, axis=0), spread[...], (((0,), (0,)), ((), ())),
            preferred_element_type=jnp.float32,
        )

    def load_group(step, g, stage):
        for p in range(ROWS):
            cell = base_s[step, g * ROWS + p]
            for k, (dx, dy) in enumerate(SQUARE):
                stage[pl.ds(g * GROUP + k * ROWS * PITCH + p, ROWS, stride=PITCH), :] = cells[
                    cell + (dx * pitch_y + dy)
                ]

    def sum_group(g, stage, wide, acc):
        here = slice(g * ROWS, g * ROWS + ROWS)
        x0, y0, z0 = (wide[here, n * LANES : (n + 1) * LANES] for n in range(3))
        xs, ys = (x0, x0 - 1.0), (y0, y0 - 1.0)
        totals = [None] * 3
        for k, (dx, dy) in enumerate(SQUARE):
            def chan(c):
                return stage[pl.ds(g * GROUP + (k * ROWS + c) * PITCH, ROWS), :]

            ex, ey, ez = chan(0) - xs[dx], chan(1) - ys[dy], chan(2) - z0
            d2 = ex * ex + ey * ey + ez * ez
            w = jnp.maximum(1.0 - d2 * INV_RADIUS_SQ, 0.0)
            for c in range(3):
                term = w * chan(3 + c)
                totals[c] = term if k == 0 else totals[c] + term
        for c in range(3):
            acc[c, here, :] = totals[c]

    def pack(step, row, acc, carry):
        span = pl.ds(pl.multiple_of(step * LANES, LANES), LANES)
        mine = own_iota == owner_v[pl.ds(row, 1), :]
        hot = jnp.where(mine, 1.0, 0.0)
        before = jnp.dot(hot.astype(jnp.bfloat16), tri[...], preferred_element_type=jnp.float32)
        rank = jnp.sum(jnp.where(mine, before + carry, 0.0), axis=0, keepdims=True)
        values = []
        for c in range(3):
            rad = jnp.sum(acc[c].T, axis=0, keepdims=True) * albedo[c : c + 1, span]
            high = rad.astype(jnp.bfloat16).astype(jnp.float32)
            values += [high, rad - high]
        for n in range(2):
            values.append(pixel_v[pl.ds(n * steps + step, 1), :].astype(jnp.float32))
        left = jnp.concatenate(
            [jnp.where(mine, v, 0.0).astype(jnp.bfloat16) for v in values], axis=0
        )
        right = jnp.where(cap_iota == rank, 1.0, 0.0).astype(jnp.bfloat16)
        return left, right, carry + jnp.sum(hot, axis=1, keepdims=True)

    def half_step(now, later, was, row, stages, wides, accs, carry):
        result = pack(was, row, accs[1], carry)
        widen(later, wides[1])
        for g in range(LANES // ROWS):
            load_group(later, g, stages[1])
            sum_group(g, stages[0], wides[0], accs[0])
        return result

    def two_steps(i, carry):
        n = 2 * i
        left_a, right_a, carry = half_step(
            n, n + 1, jnp.maximum(n - 1, 0), n + ROWS - 1,
            (stage_a, stage_b), (wide_a, wide_b), (acc_a, acc_b), carry,
        )
        left_b, right_b, carry = half_step(
            n + 1, jnp.minimum(n + 2, steps - 1), n, n + ROWS,
            (stage_b, stage_a), (wide_b, wide_a), (acc_b, acc_a), carry,
        )
        packed[...] += lax.dot_general(
            jnp.concatenate([left_a, left_b], axis=1), jnp.concatenate([right_a, right_b], axis=1),
            NT, preferred_element_type=jnp.float32,
        )
        return carry

    widen(0, wide_a)
    for g in range(LANES // ROWS):
        load_group(0, g, stage_a)
    carry = lax.fori_loop(0, steps // 2, two_steps, jnp.zeros((owners, 1), jnp.float32))
    last, right_side, _ = pack(steps - 1, steps + ROWS - 1, acc_b, carry)
    packed[...] += lax.dot_general(last, right_side, NT, preferred_element_type=jnp.float32)

    flat_send = send.reshape(owners * pitch, LANES)

    def part(v, j):
        return packed[pl.ds(v * owners, owners), pl.ds(j * LANES, LANES)]

    for j in range(cap_rows):
        for c in range(3):
            flat_send[pl.ds(c * cap_rows + j, owners, stride=pitch), :] = (
                part(2 * c, j) + part(2 * c + 1, j)
            )
        flat_send[pl.ds(3 * cap_rows + j, owners, stride=pitch), :] = (
            part(6, j) * float(LANES) + part(7, j)
        )

    def copy_to(s):
        to = lax.rem(me + s, owners)
        return pltpu.make_async_remote_copy(
            src_ref=send.at[to, pl.ds(0, used)],
            dst_ref=recv.at[me, pl.ds(0, used)],
            send_sem=send_sem.at[to],
            recv_sem=recv_sem.at[me],
            device_id=(to // ny, lax.rem(to, ny)),
            device_id_type=MESH,
        )

    def go(s, _):
        copy_to(s).start()
        return 0

    lax.fori_loop(1, owners, go, 0)
    recv[me] = send[me]

    halves = out.shape[2] // LANES
    high_rows = tiles_dev * halves
    high_iota = lax.broadcasted_iota(jnp.int32, (high_rows, LANES), 0).astype(jnp.float32)
    low_iota = lax.broadcasted_iota(jnp.int32, (LANES, LANES), 0).astype(jnp.float32)

    def arrive(s):
        come = lax.rem(me + owners - s, owners)

        @pl.when(s > 0)
        def _():
            pltpu.make_async_remote_copy(
                src_ref=send.at[come, pl.ds(0, used)],
                dst_ref=recv.at[come, pl.ds(0, used)],
                send_sem=send_sem.at[come],
                recv_sem=recv_sem.at[come],
                device_id=(come // ny, lax.rem(come, ny)),
                device_id_type=MESH,
            ).wait_recv()

        return come

    def add(step, total):
        lefts, rights = [], []
        sources = [arrive(step * 4 + u) for u in range(4)]
        for come in sources:
            blk = recv[come]
            for j in range(cap_rows):
                def row(v):
                    r = v * cap_rows + j
                    return blk[r : r + 1]

                where = row(3)
                high = jnp.floor(where * (1.0 / LANES))
                here = high_iota == high
                pieces = []
                for c in range(3):
                    value = row(c)
                    top = value.astype(jnp.bfloat16).astype(jnp.float32)
                    pieces += [jnp.where(here, top, 0.0), jnp.where(here, value - top, 0.0)]
                lefts.append(jnp.concatenate(pieces, axis=0).astype(jnp.bfloat16))
                rights.append(
                    jnp.where(low_iota == where - high * float(LANES), 1.0, 0.0).astype(jnp.bfloat16)
                )
        left = jnp.concatenate(lefts, axis=1)
        right = jnp.concatenate(rights, axis=1)
        return total + lax.dot_general(left, right, NT, preferred_element_type=jnp.float32)

    total = lax.fori_loop(0, owners // 4, add, jnp.zeros((6 * high_rows, LANES), jnp.float32))
    for c in range(3):
        for h in range(halves):
            at = 2 * c * high_rows + h * tiles_dev
            out[c, :, h * LANES : (h + 1) * LANES] = (
                total[at : at + tiles_dev] + total[at + high_rows : at + high_rows + tiles_dev]
            )

    def sent(s, _):
        copy_to(s).wait_send()
        return 0

    lax.fori_loop(1, owners, sent, 0)


def per_device(
    nx, ny, photon_data, block_counts, gather_offsets, gather_blocks, albedo, gather_pixels, tile_slot
):
    cx, cy = photon_data.shape[1:3]
    points = gather_offsets.shape[1]
    steps = points // LANES
    owners = nx * ny
    tiles = tile_slot.shape[0]
    tiles_dev = tiles // owners
    cap_rows = -(-(3 * points // owners) // LANES)
    pitch = -(-4 * cap_rows // ROWS) * ROWS
    vm = pl.BlockSpec(memory_space=pltpu.VMEM)
    smem = pl.BlockSpec(memory_space=pltpu.SMEM)
    dma, f32 = pltpu.SemaphoreType.DMA, jnp.float32
    table_rows = LANES // ROWS * GROUP
    return pl.pallas_call(
        functools.partial(whole_kernel, nx, ny, cap_rows, tiles_dev),
        out_shape=jax.ShapeDtypeStruct((3, tiles_dev, TILE_PIX), f32),
        in_specs=[pl.BlockSpec(memory_space=pl.ANY)] + [vm] * 5 + [smem],
        out_specs=vm,
        scratch_shapes=[
            pltpu.VMEM((cx + 2, cy + 2, ROWS, LANES), f32),
            pltpu.VMEM((2, cy, ROWS, LANES), f32),
            pltpu.VMEM((2, cx, ROWS, LANES), f32),
            pltpu.VMEM((table_rows, LANES), f32),
            pltpu.VMEM((table_rows, LANES), f32),
            pltpu.VMEM((LANES, 3 * LANES), f32),
            pltpu.VMEM((LANES, 3 * LANES), f32),
            pltpu.VMEM((3, LANES, LANES), f32),
            pltpu.VMEM((3, LANES, LANES), f32),
            pltpu.VMEM((3 * ROWS, 3 * LANES), jnp.bfloat16),
            pltpu.VMEM((LANES, LANES), jnp.bfloat16),
            pltpu.VMEM((cy, cx), f32),
            pltpu.VMEM((LANES, LANES), f32),
            pltpu.VMEM((ROWS, points), f32),
            pltpu.VMEM((steps, LANES), jnp.int32),
            pltpu.SMEM((steps, LANES), jnp.int32),
            pltpu.VMEM((steps + ROWS, LANES), jnp.int32),
            pltpu.VMEM((2 * steps, LANES), jnp.int32),
            pltpu.VMEM((8 * owners, cap_rows * LANES), f32),
            pltpu.VMEM((owners, pitch, LANES), f32),
            pltpu.VMEM((owners, pitch, LANES), f32),
            dma((CHANNELS,)),
            dma((4 * CHANNELS,)),
            dma,
            dma((8,)),
            dma((8,)),
            dma((owners,)),
            dma((owners,)),
        ],
        compiler_params=pltpu.CompilerParams(collective_id=0, has_side_effects=True),
        name="estimate",
    )(
        photon_data, block_counts.T, gather_offsets, gather_blocks, albedo,
        gather_pixels.reshape(steps, LANES), tile_slot,
    )


def solution(mesh):
    both = ("bx", "by")
    in_specs = (
        P(None, "bx", "by", None), P("bx", "by"), P(None, both), P(None, both),
        P(None, both), P(both), P(),
    )
    return jax.shard_map(
        functools.partial(per_device, mesh.shape["bx"], mesh.shape["by"]),
        mesh=mesh, in_specs=in_specs, out_specs=P(None, both, None), check_vma=False,
    )
```

```python
import functools

import jax
import jax.numpy as jnp
from jax import lax
from jax.experimental import pallas as pl
from jax.experimental.pallas import tpu as pltpu
from jax.sharding import PartitionSpec as P

TILE_PIX = 256
INV_RADIUS_SQ = 4.0
FAR = 1.0e4
LANES = 128
ROWS = 8
CHANNELS = 6
MESH = pl.DeviceIdType.MESH
NT = (((1,), (1,)), ((), ()))
PITCH = 9
GROUP = 2 * ROWS * PITCH


def split_by(value, size):
    if size & (size - 1) == 0:
        return value >> (size.bit_length() - 1), value & (size - 1)
    return lax.div(value, size), lax.rem(value, size)


def whole_kernel(
    nx, ny, cap_rows, tiles_dev,
    photons, counts_h, offsets_h, blocks_h, albedo_h, pixels_h, tile_slot_h, out,
    table, edge_x, edge_y, ring_y, stage_a, stage_b, wide_a, wide_b, acc_a, acc_b, partial,
    spread, tri, counts, offsets, blocks, albedo, pixels, tile_slot,
    count_row, count_col, points_v, base_v, base_s, owner_v, left_v, right_v,
    packed, packed_at, send, recv,
    fill_sem, edge_sem, small_sem, base_sem, halo_send, halo_recv, send_sem, recv_sem,
):
    cx, cy = photons.shape[1], photons.shape[2]
    pitch_y = cy + 2
    grid_x, grid_y = cx * nx, cy * ny
    points = offsets.shape[1]
    steps = points // LANES
    owners = nx * ny
    pitch = send.shape[1]
    used = 4 * cap_rows
    ix, iy = lax.axis_index("bx"), lax.axis_index("by")
    me = ix * ny + iy

    barrier = pltpu.get_barrier_semaphore()

    def greet(s, _):
        to = lax.rem(me + s, owners)
        pl.semaphore_signal(
            barrier, inc=1, device_id=(to // ny, lax.rem(to, ny)), device_id_type=MESH
        )
        return 0

    lax.fori_loop(1, owners, greet, 0)

    small = [
        pltpu.make_async_copy(src, dst, small_sem.at[n])
        for n, (src, dst) in enumerate(
            (
                (counts_h, counts), (blocks_h, blocks), (offsets_h, offsets),
                (pixels_h, pixels), (tile_slot_h, tile_slot), (albedo_h, albedo),
            )
        )
    ]
    edges = []
    for c in range(CHANNELS):
        for s, x in enumerate((cx - 1, 0)):
            edges.append(
                pltpu.make_async_copy(
                    photons.at[c, x], edge_x.at[s, :, c], edge_sem.at[len(edges)]
                )
            )
        for s, y in enumerate((cy - 1, 0)):
            edges.append(
                pltpu.make_async_copy(
                    photons.at[c, :, y], edge_y.at[s, :, c], edge_sem.at[len(edges)]
                )
            )
    fills = [
        pltpu.make_async_copy(
            photons.at[c], table.at[pl.ds(1, cx), pl.ds(1, cy), c], fill_sem.at[c]
        )
        for c in range(CHANNELS)
    ]
    small[0].start()
    for edge in edges:
        edge.start()
    for copy in small[1:]:
        copy.start()
    for fill in fills:
        fill.start()

    small[0].wait()
    count_row[...] = counts[...].astype(jnp.float32)
    square = jnp.concatenate(
        [count_row[...], jnp.zeros((cy, LANES - cx), jnp.float32)], axis=1
    )
    square = jnp.concatenate([square, jnp.zeros((LANES - cy, LANES), jnp.float32)], axis=0)
    count_col[...] = square.T
    lane = lax.broadcasted_iota(jnp.int32, (ROWS, LANES), 1).astype(jnp.float32)

    def hide(ref, first, column):
        rows = column.shape[0]
        for r in range(0, rows, ROWS):
            place = pl.ds(first + r * ROWS, ROWS, stride=ROWS)
            ref[place, :] = jnp.where(lane < column[r : r + ROWS], ref[place, :], FAR)

    for edge in edges:
        edge.wait()
    flat_x = edge_x.reshape(2 * cy * ROWS, LANES)
    flat_y = edge_y.reshape(2 * cx * ROWS, LANES)
    for s, y in enumerate((cy - 1, 0)):
        hide(flat_y, s * cx * ROWS, count_col[0:cx, y : y + 1])
    for s, x in enumerate((cx - 1, 0)):
        hide(flat_x, s * cy * ROWS, count_row[:, x : x + 1])
    pl.semaphore_wait(barrier, owners - 1)

    right, left = lax.rem(ix + 1, nx), lax.rem(ix + nx - 1, nx)
    up, down = lax.rem(iy + 1, ny), lax.rem(iy + ny - 1, ny)
    data = pl.ds(0, CHANNELS)
    wide_x, wide_y = pl.ds(1, cx), pl.ds(1, cy)
    parts = [
        (edge_y.at[0, :, data], ring_y.at[0, wide_x, data], ix, up),
        (edge_y.at[1, :, data], ring_y.at[1, wide_x, data], ix, down),
        (edge_x.at[0, :, data], table.at[0, wide_y, data], right, iy),
        (edge_x.at[1, :, data], table.at[cx + 1, wide_y, data], left, iy),
        (edge_x.at[0, cy - 1, data], ring_y.at[0, 0, data], right, up),
        (edge_x.at[0, 0, data], ring_y.at[1, 0, data], right, down),
        (edge_x.at[1, cy - 1, data], ring_y.at[0, cx + 1, data], left, up),
        (edge_x.at[1, 0, data], ring_y.at[1, cx + 1, data], left, down),
    ]
    halos = [
        pltpu.make_async_remote_copy(
            src_ref=src, dst_ref=dst, send_sem=halo_send.at[n], recv_sem=halo_recv.at[n],
            device_id=(px, py), device_id_type=MESH,
        )
        for n, (src, dst, px, py) in enumerate(parts)
    ]
    for halo in halos:
        halo.start()

    for copy in small[1:4]:
        copy.wait()
    cell_x, cell_y = split_by(blocks[...], grid_y)

    def local(cell, first, size):
        t = cell - first + 1
        t = jnp.where(t < 0, t + size, t)
        return jnp.where(t >= size, t - size, t)

    lx, ly = local(cell_x, ix * cx, grid_x), local(cell_y, iy * cy, grid_y)
    low_x, low_y = jnp.min(lx, axis=0, keepdims=True), jnp.min(ly, axis=0, keepdims=True)
    own_y = ly[0:1]
    other_y = 2 * low_y + 1 - own_y
    line = jnp.minimum(low_x, cx) * pitch_y
    bases = (
        line + jnp.clip(own_y, 0, cy + 1),
        line + jnp.clip(other_y, 0, cy + 1),
    )
    for n in range(2):
        for j in range(steps):
            base_v[n * steps + j : n * steps + j + 1, :] = bases[n][:, j * LANES : (j + 1) * LANES]
    to_scalar = pltpu.make_async_copy(base_v, base_s, base_sem)
    to_scalar.start()
    points_v[...] = jnp.zeros_like(points_v)
    points_v[0:1, :] = offsets[0:1, :] + (lx[0:1] - low_x).astype(jnp.float32)
    points_v[1:2, :] = offsets[1:2, :]
    points_v[2:3, :] = offsets[2:3, :]
    points_v[3:4, :] = offsets[1:2, :] + (own_y - other_y).astype(jnp.float32)

    tile, within = split_by(pixels[...], TILE_PIX)
    small[4].wait()

    def look_up(t, found):
        for u in range(ROWS):
            n = t * ROWS + u
            found = jnp.where(tile == n, tile_slot[n], found)
        return found

    slot = lax.fori_loop(0, tile_slot.shape[0] // ROWS, look_up, jnp.zeros_like(tile))
    owner, place = split_by(slot, tiles_dev)
    half, low = split_by(within, LANES)
    first = half * tiles_dev + place
    owner_v[...] = jnp.full(owner_v.shape, -1, jnp.int32)
    owner_v[pl.ds(ROWS, steps), :] = owner

    a = lax.broadcasted_iota(jnp.int32, (LANES, LANES), 0)
    b = lax.broadcasted_iota(jnp.int32, (LANES, LANES), 1)
    tri[...] = jnp.where(a < b, 1.0, 0.0).astype(jnp.bfloat16)
    for n, rows in enumerate(((0, 1, 2), (0, 3, 2))):
        a = lax.broadcasted_iota(jnp.int32, spread.shape[1:], 0) % ROWS
        b = lax.broadcasted_iota(jnp.int32, spread.shape[1:], 1) // LANES
        hit = (a == rows[0]) & (b == 0)
        for m in range(1, 3):
            hit = hit | ((a == rows[m]) & (b == m))
        spread[n] = jnp.where(hit, 1.0, 0.0).astype(jnp.bfloat16)
    packed[...] = jnp.zeros_like(packed)
    acc_b[...] = jnp.zeros_like(acc_b)

    own_iota = lax.broadcasted_iota(jnp.int32, (owners, LANES), 0)
    cap_iota = lax.broadcasted_iota(jnp.int32, (cap_rows * LANES, LANES), 0).astype(jnp.float32)
    nothing = jnp.zeros((2 * owners, LANES), jnp.bfloat16)
    empty = jnp.zeros((cap_rows * LANES, LANES), jnp.bfloat16)
    for at in (0, steps + 1):
        left_v[:, at * LANES : (at + 1) * LANES] = nothing
        right_v[:, at * LANES : (at + 1) * LANES] = empty
    carry = jnp.zeros((owners, LANES), jnp.float32)
    ones = jnp.ones((LANES, LANES), jnp.bfloat16)
    for j in range(steps):
        mine = own_iota == owner[j : j + 1, :]
        hot = jnp.where(mine, 1.0, 0.0).astype(jnp.bfloat16)
        before = jnp.dot(hot, tri[...], preferred_element_type=jnp.float32)
        rank = jnp.sum(jnp.where(mine, before + carry, 0.0), axis=0, keepdims=True)
        carry = carry + jnp.dot(hot, ones, preferred_element_type=jnp.float32)
        span = slice((j + 1) * LANES, (j + 2) * LANES)
        left_v[:, span] = jnp.concatenate(
            [
                jnp.where(mine, v[j : j + 1, :].astype(jnp.float32), 0.0).astype(jnp.bfloat16)
                for v in (first, low)
            ],
            axis=0,
        )
        right_v[:, span] = jnp.where(cap_iota == rank, 1.0, 0.0).astype(jnp.bfloat16)
    packed_at[...] = lax.dot_general(
        left_v[...], right_v[...], NT, preferred_element_type=jnp.float32
    )

    for fill in fills:
        fill.wait()
    flat = table.reshape((cx + 2) * pitch_y * ROWS, LANES)
    cells = table.reshape((cx + 2) * pitch_y, ROWS, LANES)
    for x in range(cx):
        hide(flat, ((x + 1) * pitch_y + 1) * ROWS, count_row[:, x : x + 1])
    small[5].wait()
    to_scalar.wait()

    def widen(n, step, wide):
        value = points_v[:, pl.ds(pl.multiple_of(step * LANES, LANES), LANES)]
        pieces = []
        for _ in range(3):
            high = value.astype(jnp.bfloat16)
            pieces.append(high)
            value = value - high.astype(jnp.float32)
        wide[...] = lax.dot_general(
            jnp.concatenate(pieces, axis=0), spread[n], (((0,), (0,)), ((), ())),
            preferred_element_type=jnp.float32,
        )

    def load_group(n, step, g, stage):
        for p in range(ROWS):
            cell = base_s[n * steps + step, g * ROWS + p]
            for k in range(2):
                stage[pl.ds(g * GROUP + k * ROWS * PITCH + p, ROWS, stride=PITCH), :] = cells[
                    cell + k * pitch_y
                ]

    def sum_group(g, stage, wide, totals):
        here = slice(g * ROWS, g * ROWS + ROWS)
        x0, y0, z0 = (wide[here, n * LANES : (n + 1) * LANES] for n in range(3))
        for k, x in enumerate((x0, x0 - 1.0)):
            def chan(c):
                return stage[pl.ds(g * GROUP + (k * ROWS + c) * PITCH, ROWS), :]

            ex, ey, ez = chan(0) - x, chan(1) - y0, chan(2) - z0
            d2 = ex * ex + ey * ey + ez * ez
            w = jnp.maximum(1.0 - d2 * INV_RADIUS_SQ, 0.0)
            for c in range(3):
                term = w * chan(3 + c)
                totals[c] = term if totals[c] is None else totals[c] + term
        return totals

    def first_half(now, later, stages, wides):
        widen(0, later, wides[1])
        for g in range(LANES // ROWS):
            load_group(0, later, g, stages[1])
            totals = sum_group(g, stages[0], wides[0], [None] * 3)
            for c in range(3):
                partial[now, c, g * ROWS : (g + 1) * ROWS, :] = totals[c]

    def first_two(i, _):
        n = 2 * i
        first_half(n, n + 1, (stage_a, stage_b), (wide_a, wide_b))
        first_half(n + 1, jnp.minimum(n + 2, steps - 1), (stage_b, stage_a), (wide_b, wide_a))
        return 0

    for halo in halos[2:4]:
        halo.wait()
    widen(0, 0, wide_a)
    for g in range(LANES // ROWS):
        load_group(0, 0, g, stage_a)
    lax.fori_loop(0, steps // 2, first_two, 0)

    for halo in halos[:2] + halos[4:]:
        halo.wait()
    for s, y in enumerate((0, cy + 1)):
        for x in range(cx + 2):
            table[x, y] = ring_y[s, x]

    def radiance(step, acc):
        span = pl.ds(pl.multiple_of(step * LANES, LANES), LANES)
        return [
            jnp.sum(acc[c].T, axis=0, keepdims=True) * albedo[c : c + 1, span] for c in range(3)
        ]

    def pack(row, values):
        mine = own_iota == owner_v[pl.ds(row, 1), :]
        pieces = []
        for rad in values:
            high = rad.astype(jnp.bfloat16).astype(jnp.float32)
            pieces += [high, rad - high]
        return jnp.concatenate(
            [jnp.where(mine, v, 0.0).astype(jnp.bfloat16) for v in pieces], axis=0
        )

    def second_half(now, later, was, row, stages, wides, accs):
        side = pack(row, radiance(was, accs[1]))
        widen(1, later, wides[1])
        for g in range(LANES // ROWS):
            load_group(1, later, g, stages[1])
            here = slice(g * ROWS, (g + 1) * ROWS)
            totals = sum_group(g, stages[0], wides[0], [partial[now, c, here, :] for c in range(3)])
            for c in range(3):
                accs[0][c, here, :] = totals[c]
        return side

    def add_packed(sides, pair, width):
        span = pl.ds(pl.multiple_of(pair * 2 * LANES, LANES), width)
        packed[...] += lax.dot_general(
            jnp.concatenate(sides, axis=1), right_v[:, span], NT, preferred_element_type=jnp.float32
        )

    def second_two(i, _):
        n = 2 * i
        side_a = second_half(
            n, n + 1, jnp.maximum(n - 1, 0), n + ROWS - 1,
            (stage_a, stage_b), (wide_a, wide_b), (acc_a, acc_b),
        )
        side_b = second_half(
            n + 1, jnp.minimum(n + 2, steps - 1), n, n + ROWS,
            (stage_b, stage_a), (wide_b, wide_a), (acc_b, acc_a),
        )
        add_packed([side_a, side_b], i, 2 * LANES)
        return 0

    widen(1, 0, wide_a)
    for g in range(LANES // ROWS):
        load_group(1, 0, g, stage_a)
    lax.fori_loop(0, steps // 2, second_two, 0)
    add_packed([pack(steps + ROWS - 1, radiance(steps - 1, acc_b))], steps // 2, LANES)

    flat_send = send.reshape(owners * pitch, LANES)

    def part(v, j):
        return packed[pl.ds(v * owners, owners), pl.ds(j * LANES, LANES)]

    for j in range(cap_rows):
        for c in range(3):
            flat_send[pl.ds(c * cap_rows + j, owners, stride=pitch), :] = (
                part(2 * c, j) + part(2 * c + 1, j)
            )
        flat_send[pl.ds(3 * cap_rows + j, owners, stride=pitch), :] = (
            packed_at[0:owners, j * LANES : (j + 1) * LANES] * float(LANES)
            + packed_at[owners : 2 * owners, j * LANES : (j + 1) * LANES]
        )

    def copy_to(s):
        to = lax.rem(me + s, owners)
        return pltpu.make_async_remote_copy(
            src_ref=send.at[to, pl.ds(0, used)],
            dst_ref=recv.at[me, pl.ds(0, used)],
            send_sem=send_sem.at[to],
            recv_sem=recv_sem.at[me],
            device_id=(to // ny, lax.rem(to, ny)),
            device_id_type=MESH,
        )

    def go(s, _):
        copy_to(s).start()
        return 0

    lax.fori_loop(1, owners, go, 0)
    recv[me] = send[me]

    halves = out.shape[2] // LANES
    high_rows = tiles_dev * halves
    high_iota = lax.broadcasted_iota(jnp.int32, (high_rows, LANES), 0).astype(jnp.float32)
    low_iota = lax.broadcasted_iota(jnp.int32, (LANES, LANES), 0).astype(jnp.float32)

    def arrive(s):
        come = lax.rem(me + owners - s, owners)

        @pl.when(s > 0)
        def _():
            pltpu.make_async_remote_copy(
                src_ref=send.at[come, pl.ds(0, used)],
                dst_ref=recv.at[come, pl.ds(0, used)],
                send_sem=send_sem.at[come],
                recv_sem=recv_sem.at[come],
                device_id=(come // ny, lax.rem(come, ny)),
                device_id_type=MESH,
            ).wait_recv()

        return come

    def add(step, total):
        lefts, rights = [], []
        sources = [arrive(step * 4 + u) for u in range(4)]
        for come in sources:
            blk = recv[come]
            for j in range(cap_rows):
                def row(v):
                    r = v * cap_rows + j
                    return blk[r : r + 1]

                where = row(3)
                high = jnp.floor(where * (1.0 / LANES))
                here = high_iota == high
                pieces = []
                for c in range(3):
                    value = row(c)
                    top = value.astype(jnp.bfloat16).astype(jnp.float32)
                    pieces += [jnp.where(here, top, 0.0), jnp.where(here, value - top, 0.0)]
                lefts.append(jnp.concatenate(pieces, axis=0).astype(jnp.bfloat16))
                rights.append(
                    jnp.where(low_iota == where - high * float(LANES), 1.0, 0.0).astype(jnp.bfloat16)
                )
        left = jnp.concatenate(lefts, axis=1)
        right = jnp.concatenate(rights, axis=1)
        return total + lax.dot_general(left, right, NT, preferred_element_type=jnp.float32)

    total = lax.fori_loop(0, owners // 4, add, jnp.zeros((6 * high_rows, LANES), jnp.float32))
    for c in range(3):
        for h in range(halves):
            at = 2 * c * high_rows + h * tiles_dev
            out[c, :, h * LANES : (h + 1) * LANES] = (
                total[at : at + tiles_dev] + total[at + high_rows : at + high_rows + tiles_dev]
            )

    def sent(s, _):
        copy_to(s).wait_send()
        return 0

    lax.fori_loop(1, owners, sent, 0)


def per_device(
    nx, ny, photon_data, block_counts, gather_offsets, gather_blocks, albedo, gather_pixels, tile_slot
):
    cx, cy = photon_data.shape[1:3]
    points = gather_offsets.shape[1]
    steps = points // LANES
    owners = nx * ny
    tiles = tile_slot.shape[0]
    tiles_dev = tiles // owners
    cap_rows = -(-(3 * points // owners) // LANES)
    pitch = -(-4 * cap_rows // ROWS) * ROWS
    hb, vm = pl.BlockSpec(memory_space=pl.ANY), pl.BlockSpec(memory_space=pltpu.VMEM)
    dma, f32, i32, bf16 = pltpu.SemaphoreType.DMA, jnp.float32, jnp.int32, jnp.bfloat16
    stage_rows = LANES // ROWS * GROUP
    return pl.pallas_call(
        functools.partial(whole_kernel, nx, ny, cap_rows, tiles_dev),
        out_shape=jax.ShapeDtypeStruct((3, tiles_dev, TILE_PIX), f32),
        in_specs=[hb] * 7,
        out_specs=vm,
        scratch_shapes=[
            pltpu.VMEM((cx + 2, cy + 2, ROWS, LANES), f32),
            pltpu.VMEM((2, cy, ROWS, LANES), f32),
            pltpu.VMEM((2, cx, ROWS, LANES), f32),
            pltpu.VMEM((2, cx + 2, ROWS, LANES), f32),
            pltpu.VMEM((stage_rows, LANES), f32),
            pltpu.VMEM((stage_rows, LANES), f32),
            pltpu.VMEM((LANES, 3 * LANES), f32),
            pltpu.VMEM((LANES, 3 * LANES), f32),
            pltpu.VMEM((3, LANES, LANES), f32),
            pltpu.VMEM((3, LANES, LANES), f32),
            pltpu.VMEM((steps, 3, LANES, LANES), f32),
            pltpu.VMEM((2, 3 * ROWS, 3 * LANES), bf16),
            pltpu.VMEM((LANES, LANES), bf16),
            pltpu.VMEM((cy, cx), i32),
            pltpu.VMEM((3, points), f32),
            pltpu.VMEM((4, points), i32),
            pltpu.VMEM((3, points), f32),
            pltpu.VMEM((steps, LANES), i32),
            pltpu.SMEM((tiles,), i32),
            pltpu.VMEM((cy, cx), f32),
            pltpu.VMEM((LANES, LANES), f32),
            pltpu.VMEM((ROWS, points), f32),
            pltpu.VMEM((2 * steps, LANES), i32),
            pltpu.SMEM((2 * steps, LANES), i32),
            pltpu.VMEM((steps + ROWS, LANES), i32),
            pltpu.VMEM((2 * owners, points + 2 * LANES), bf16),
            pltpu.VMEM((cap_rows * LANES, points + 2 * LANES), bf16),
            pltpu.VMEM((6 * owners, cap_rows * LANES), f32),
            pltpu.VMEM((2 * owners, cap_rows * LANES), f32),
            pltpu.VMEM((owners, pitch, LANES), f32),
            pltpu.VMEM((owners, pitch, LANES), f32),
            dma((CHANNELS,)),
            dma((4 * CHANNELS,)),
            dma((6,)),
            dma,
            dma((8,)),
            dma((8,)),
            dma((owners,)),
            dma((owners,)),
        ],
        compiler_params=pltpu.CompilerParams(collective_id=0, has_side_effects=True),
        name="estimate",
    )(
        photon_data, block_counts.T, gather_offsets, gather_blocks, albedo,
        gather_pixels.reshape(steps, LANES), tile_slot,
    )


def solution(mesh):
    both = ("bx", "by")
    in_specs = (
        P(None, "bx", "by", None), P("bx", "by"), P(None, both), P(None, both),
        P(None, both), P(both), P(),
    )
    return jax.shard_map(
        functools.partial(per_device, mesh.shape["bx"], mesh.shape["by"]),
        mesh=mesh, in_specs=in_specs, out_specs=P(None, both, None), check_vma=False,
    )
```

```python
import functools

import jax
import jax.numpy as jnp
from jax import lax
from jax.experimental import pallas as pl
from jax.experimental.pallas import tpu as pltpu
from jax.sharding import PartitionSpec as P

TILE_PIX = 256
INV_RADIUS_SQ = 4.0
FAR = 1.0e4
LANES = 128
ROWS = 8
CHANNELS = 6
MESH = pl.DeviceIdType.MESH
NT = (((1,), (1,)), ((), ()))
PITCH = 9
GROUP = 2 * ROWS * PITCH


def split_by(value, size):
    if size & (size - 1) == 0:
        return value >> (size.bit_length() - 1), value & (size - 1)
    return lax.div(value, size), lax.rem(value, size)


def whole_kernel(
    nx, ny, cap_rows, tiles_dev,
    photons, counts_h, offsets_h, blocks_h, albedo_h, pixels_h, tile_slot_h, out,
    table, edge_x, edge_y, ring_y, stage_a, stage_b, wide_a, wide_b, side_v, partial,
    spread, tri, counts, offsets, blocks, albedo, pixels, tile_slot,
    count_row, count_col, points_v, base_v, base_s, owner_v, left_v, right_v,
    packed, send, recv, send_at, recv_at,
    fill_sem, edge_sem, small_sem, base_sem, halo_send, halo_recv, send_sem, recv_sem,
    at_send_sem, at_recv_sem,
):
    cx, cy = photons.shape[1], photons.shape[2]
    pitch_y = cy + 2
    grid_x, grid_y = cx * nx, cy * ny
    points = offsets.shape[1]
    steps = points // LANES
    owners = nx * ny
    pitch = send.shape[1]
    ix, iy = lax.axis_index("bx"), lax.axis_index("by")
    me = ix * ny + iy

    barrier = pltpu.get_barrier_semaphore()

    def greet(s, _):
        to = lax.rem(me + s, owners)
        pl.semaphore_signal(
            barrier, inc=1, device_id=(to // ny, lax.rem(to, ny)), device_id_type=MESH
        )
        return 0

    lax.fori_loop(1, owners, greet, 0)

    small = [
        pltpu.make_async_copy(src, dst, small_sem.at[n])
        for n, (src, dst) in enumerate(
            (
                (counts_h, counts), (blocks_h, blocks), (offsets_h, offsets),
                (pixels_h, pixels), (tile_slot_h, tile_slot), (albedo_h, albedo),
            )
        )
    ]
    edges = []
    for c in range(CHANNELS):
        for s, x in enumerate((cx - 1, 0)):
            edges.append(
                pltpu.make_async_copy(
                    photons.at[c, x], edge_x.at[s, :, c], edge_sem.at[len(edges)]
                )
            )
        for s, y in enumerate((cy - 1, 0)):
            edges.append(
                pltpu.make_async_copy(
                    photons.at[c, :, y], edge_y.at[s, :, c], edge_sem.at[len(edges)]
                )
            )
    fills = [
        pltpu.make_async_copy(
            photons.at[c], table.at[pl.ds(1, cx), pl.ds(1, cy), c], fill_sem.at[c]
        )
        for c in range(CHANNELS)
    ]
    small[0].start()
    for edge in edges:
        edge.start()
    for copy in small[1:]:
        copy.start()
    for fill in fills:
        fill.start()

    small[0].wait()
    count_row[...] = counts[...].astype(jnp.float32)
    square = jnp.concatenate(
        [count_row[...], jnp.zeros((cy, LANES - cx), jnp.float32)], axis=1
    )
    square = jnp.concatenate([square, jnp.zeros((LANES - cy, LANES), jnp.float32)], axis=0)
    count_col[...] = square.T
    lane = lax.broadcasted_iota(jnp.int32, (ROWS, LANES), 1).astype(jnp.float32)

    def hide(ref, first, column):
        rows = column.shape[0]
        for r in range(0, rows, ROWS):
            place = pl.ds(first + r * ROWS, ROWS, stride=ROWS)
            ref[place, :] = jnp.where(lane < column[r : r + ROWS], ref[place, :], FAR)

    for edge in edges:
        edge.wait()
    flat_x = edge_x.reshape(2 * cy * ROWS, LANES)
    flat_y = edge_y.reshape(2 * cx * ROWS, LANES)
    for s, y in enumerate((cy - 1, 0)):
        hide(flat_y, s * cx * ROWS, count_col[0:cx, y : y + 1])
    for s, x in enumerate((cx - 1, 0)):
        hide(flat_x, s * cy * ROWS, count_row[:, x : x + 1])
    pl.semaphore_wait(barrier, owners - 1)

    right, left = lax.rem(ix + 1, nx), lax.rem(ix + nx - 1, nx)
    up, down = lax.rem(iy + 1, ny), lax.rem(iy + ny - 1, ny)
    data = pl.ds(0, CHANNELS)
    wide_x, wide_y = pl.ds(1, cx), pl.ds(1, cy)
    parts = [
        (edge_y.at[0, :, data], ring_y.at[0, wide_x, data], ix, up),
        (edge_y.at[1, :, data], ring_y.at[1, wide_x, data], ix, down),
        (edge_x.at[0, :, data], table.at[0, wide_y, data], right, iy),
        (edge_x.at[1, :, data], table.at[cx + 1, wide_y, data], left, iy),
        (edge_x.at[0, cy - 1, data], ring_y.at[0, 0, data], right, up),
        (edge_x.at[0, 0, data], ring_y.at[1, 0, data], right, down),
        (edge_x.at[1, cy - 1, data], ring_y.at[0, cx + 1, data], left, up),
        (edge_x.at[1, 0, data], ring_y.at[1, cx + 1, data], left, down),
    ]
    halos = [
        pltpu.make_async_remote_copy(
            src_ref=src, dst_ref=dst, send_sem=halo_send.at[n], recv_sem=halo_recv.at[n],
            device_id=(px, py), device_id_type=MESH,
        )
        for n, (src, dst, px, py) in enumerate(parts)
    ]
    for halo in halos:
        halo.start()

    for copy in small[1:4]:
        copy.wait()
    cell_x, cell_y = split_by(blocks[...], grid_y)

    def local(cell, first, size):
        t = cell - first + 1
        t = jnp.where(t < 0, t + size, t)
        return jnp.where(t >= size, t - size, t)

    lx, ly = local(cell_x, ix * cx, grid_x), local(cell_y, iy * cy, grid_y)
    low_x, low_y = jnp.min(lx, axis=0, keepdims=True), jnp.min(ly, axis=0, keepdims=True)
    own_y = ly[0:1]
    other_y = 2 * low_y + 1 - own_y
    line = jnp.minimum(low_x, cx) * pitch_y
    bases = (
        line + jnp.clip(own_y, 0, cy + 1),
        line + jnp.clip(other_y, 0, cy + 1),
    )
    for n in range(2):
        for j in range(steps):
            base_v[n * steps + j : n * steps + j + 1, :] = bases[n][:, j * LANES : (j + 1) * LANES]
    to_scalar = pltpu.make_async_copy(base_v, base_s, base_sem)
    to_scalar.start()
    points_v[...] = jnp.zeros_like(points_v)
    points_v[0:1, :] = offsets[0:1, :] + (lx[0:1] - low_x).astype(jnp.float32)
    points_v[1:2, :] = offsets[1:2, :]
    points_v[2:3, :] = offsets[2:3, :]
    points_v[3:4, :] = offsets[1:2, :] + (own_y - other_y).astype(jnp.float32)

    tile, within = split_by(pixels[...], TILE_PIX)
    small[4].wait()

    def look_up(t, found):
        for u in range(ROWS):
            n = t * ROWS + u
            found = jnp.where(tile == n, tile_slot[n], found)
        return found

    slot = lax.fori_loop(0, tile_slot.shape[0] // ROWS, look_up, jnp.zeros_like(tile))
    owner, place = split_by(slot, tiles_dev)
    half, low = split_by(within, LANES)
    first = half * tiles_dev + place
    owner_v[...] = jnp.full(owner_v.shape, -1, jnp.int32)
    owner_v[2 : 2 + steps, :] = owner

    a = lax.broadcasted_iota(jnp.int32, (LANES, LANES), 0)
    b = lax.broadcasted_iota(jnp.int32, (LANES, LANES), 1)
    tri[...] = jnp.where(a < b, 1.0, 0.0).astype(jnp.bfloat16)
    for n, rows in enumerate(((0, 1, 2), (0, 3, 2))):
        a = lax.broadcasted_iota(jnp.int32, spread.shape[1:], 0) % ROWS
        b = lax.broadcasted_iota(jnp.int32, spread.shape[1:], 1) // LANES
        hit = (a == rows[0]) & (b == 0)
        for m in range(1, 3):
            hit = hit | ((a == rows[m]) & (b == m))
        spread[n] = jnp.where(hit, 1.0, 0.0).astype(jnp.bfloat16)
    packed[...] = jnp.zeros_like(packed)
    side_v[...] = jnp.zeros_like(side_v)

    own_iota = lax.broadcasted_iota(jnp.int32, (owners, LANES), 0)
    cap_iota = lax.broadcasted_iota(jnp.int32, (cap_rows * LANES, LANES), 0).astype(jnp.float32)
    carry = jnp.zeros((owners, LANES), jnp.float32)
    ones = jnp.ones((LANES, LANES), jnp.bfloat16)
    for j in range(steps):
        mine = own_iota == owner[j : j + 1, :]
        hot = jnp.where(mine, 1.0, 0.0).astype(jnp.bfloat16)
        before = jnp.dot(hot, tri[...], preferred_element_type=jnp.float32)
        rank = jnp.sum(jnp.where(mine, before + carry, 0.0), axis=0, keepdims=True)
        carry = carry + jnp.dot(hot, ones, preferred_element_type=jnp.float32)
        span = slice(j * LANES, (j + 1) * LANES)
        left_v[:, span] = jnp.concatenate(
            [
                jnp.where(mine, v[j : j + 1, :].astype(jnp.float32), 0.0).astype(jnp.bfloat16)
                for v in (first, low)
            ],
            axis=0,
        )
        right_v[:, span] = jnp.where(cap_iota == rank, 1.0, 0.0).astype(jnp.bfloat16)
    packed_at = lax.dot_general(left_v[...], right_v[...], NT, preferred_element_type=jnp.float32)
    packed_at = packed_at[:owners] * float(LANES) + packed_at[owners:]
    flat_at = send_at.reshape(owners * send_at.shape[1], LANES)
    for j in range(cap_rows):
        flat_at[pl.ds(j, owners, stride=send_at.shape[1]), :] = packed_at[
            :, j * LANES : (j + 1) * LANES
        ]

    for fill in fills:
        fill.wait()
    flat = table.reshape((cx + 2) * pitch_y * ROWS, LANES)
    cells = table.reshape((cx + 2) * pitch_y, ROWS, LANES)
    for x in range(cx):
        hide(flat, ((x + 1) * pitch_y + 1) * ROWS, count_row[:, x : x + 1])
    small[5].wait()
    to_scalar.wait()

    def widen(n, step, wide):
        value = points_v[:, pl.ds(pl.multiple_of(step * LANES, LANES), LANES)]
        pieces = []
        for _ in range(3):
            high = value.astype(jnp.bfloat16)
            pieces.append(high)
            value = value - high.astype(jnp.float32)
        wide[...] = lax.dot_general(
            jnp.concatenate(pieces, axis=0), spread[n], (((0,), (0,)), ((), ())),
            preferred_element_type=jnp.float32,
        )

    def load_group(n, step, g, stage):
        for p in range(ROWS):
            cell = base_s[n * steps + step, g * ROWS + p]
            for k in range(2):
                stage[pl.ds(g * GROUP + k * ROWS * PITCH + p, ROWS, stride=PITCH), :] = cells[
                    cell + k * pitch_y
                ]

    def sum_group(g, stage, wide, totals):
        here = slice(g * ROWS, g * ROWS + ROWS)
        x0, y0, z0 = (wide[here, n * LANES : (n + 1) * LANES] for n in range(3))
        for k, x in enumerate((x0, x0 - 1.0)):
            def chan(c):
                return stage[pl.ds(g * GROUP + (k * ROWS + c) * PITCH, ROWS), :]

            ex, ey, ez = chan(0) - x, chan(1) - y0, chan(2) - z0
            d2 = ex * ex + ey * ey + ez * ez
            w = jnp.maximum(1.0 - d2 * INV_RADIUS_SQ, 0.0)
            for c in range(3):
                term = w * chan(3 + c)
                totals[c] = term if totals[c] is None else totals[c] + term
        return totals

    def first_half(now, later, stages, wides):
        widen(0, later, wides[1])
        for g in range(LANES // ROWS):
            load_group(0, later, g, stages[1])
            totals = sum_group(g, stages[0], wides[0], [None] * 3)
            for c in range(3):
                partial[now + 2, c, g * ROWS : (g + 1) * ROWS, :] = totals[c]

    def first_two(i, _):
        n = 2 * i
        first_half(n, n + 1, (stage_a, stage_b), (wide_a, wide_b))
        first_half(n + 1, jnp.minimum(n + 2, steps - 1), (stage_b, stage_a), (wide_b, wide_a))
        return 0

    for halo in halos[2:4]:
        halo.wait()
    widen(0, 0, wide_a)
    for g in range(LANES // ROWS):
        load_group(0, 0, g, stage_a)
    lax.fori_loop(0, steps // 2, first_two, 0)

    for halo in halos[:2] + halos[4:]:
        halo.wait()
    for s, y in enumerate((0, cy + 1)):
        for x in range(cx + 2):
            table[x, y] = ring_y[s, x]

    def copy_to(s, rows, source, target, sems):
        to = lax.rem(me + s, owners)
        return pltpu.make_async_remote_copy(
            src_ref=source.at[to, pl.ds(0, rows)],
            dst_ref=target.at[me, pl.ds(0, rows)],
            send_sem=sems[0].at[to],
            recv_sem=sems[1].at[me],
            device_id=(to // ny, lax.rem(to, ny)),
            device_id_type=MESH,
        )

    places = (cap_rows, send_at, recv_at, (at_send_sem, at_recv_sem))
    amounts = (3 * cap_rows, send, recv, (send_sem, recv_sem))

    def go_places(s, _):
        copy_to(s, *places).start()
        return 0

    lax.fori_loop(1, owners, go_places, 0)

    def pack(row, index, step):
        mine = own_iota == owner_v[pl.ds(row, 1), :]
        span = pl.ds(pl.multiple_of(step * LANES, LANES), LANES)
        pieces = []
        for c in range(3):
            rad = jnp.sum(partial[index, c].T, axis=0, keepdims=True) * albedo[c : c + 1, span]
            high = rad.astype(jnp.bfloat16).astype(jnp.float32)
            pieces += [high, rad - high]
        return jnp.concatenate(
            [jnp.where(mine, v, 0.0).astype(jnp.bfloat16) for v in pieces], axis=0
        )

    def second_half(now, later, stages, wides):
        widen(1, later, wides[1])
        for g in range(LANES // ROWS):
            load_group(1, later, g, stages[1])
            here = slice(g * ROWS, (g + 1) * ROWS)
            totals = sum_group(
                g, stages[0], wides[0], [partial[now + 2, c, here, :] for c in range(3)]
            )
            for c in range(3):
                partial[now + 2, c, here, :] = totals[c]

    def second_two(i, _):
        n = 2 * i
        span = pl.ds(pl.multiple_of(jnp.maximum(n - 4, 0) * LANES, LANES), 2 * LANES)
        packed[...] += lax.dot_general(
            side_v[...], right_v[:, span], NT, preferred_element_type=jnp.float32
        )
        for u in range(2):
            side_v[:, u * LANES : (u + 1) * LANES] = pack(n + u, n + u, jnp.maximum(n - 2, 0) + u)
        second_half(n, n + 1, (stage_a, stage_b), (wide_a, wide_b))
        second_half(n + 1, jnp.minimum(n + 2, steps - 1), (stage_b, stage_a), (wide_b, wide_a))
        return 0

    widen(1, 0, wide_a)
    for g in range(LANES // ROWS):
        load_group(1, 0, g, stage_a)
    lax.fori_loop(0, steps // 2, second_two, 0)
    sides = [side_v[...]] + [pack(steps + u, steps + u, steps - 2 + u) for u in range(2)]
    packed[...] += lax.dot_general(
        jnp.concatenate(sides, axis=1), right_v[:, (steps - 4) * LANES :], NT,
        preferred_element_type=jnp.float32,
    )

    flat_send = send.reshape(owners * pitch, LANES)

    def part(v, j):
        return packed[pl.ds(v * owners, owners), pl.ds(j * LANES, LANES)]

    for j in range(cap_rows):
        for c in range(3):
            flat_send[pl.ds(c * cap_rows + j, owners, stride=pitch), :] = (
                part(2 * c, j) + part(2 * c + 1, j)
            )

    def go(s, _):
        copy_to(s, *amounts).start()
        return 0

    lax.fori_loop(1, owners, go, 0)
    recv[me] = send[me]
    recv_at[me] = send_at[me]

    halves = out.shape[2] // LANES
    high_rows = tiles_dev * halves
    high_iota = lax.broadcasted_iota(jnp.int32, (high_rows, LANES), 0).astype(jnp.float32)
    low_iota = lax.broadcasted_iota(jnp.int32, (LANES, LANES), 0).astype(jnp.float32)

    def arrive(s):
        come = lax.rem(me + owners - s, owners)

        @pl.when(s > 0)
        def _():
            for rows, source, target, sems in (places, amounts):
                pltpu.make_async_remote_copy(
                    src_ref=source.at[come, pl.ds(0, rows)],
                    dst_ref=target.at[come, pl.ds(0, rows)],
                    send_sem=sems[0].at[come],
                    recv_sem=sems[1].at[come],
                    device_id=(come // ny, lax.rem(come, ny)),
                    device_id_type=MESH,
                ).wait_recv()

        return come

    def add(step, total):
        lefts, rights = [], []
        sources = [arrive(step * 4 + u) for u in range(4)]
        for come in sources:
            blk, spots = recv[come], recv_at[come]
            for j in range(cap_rows):
                def row(v):
                    r = v * cap_rows + j
                    return blk[r : r + 1]

                where = spots[j : j + 1]
                high = jnp.floor(where * (1.0 / LANES))
                here = high_iota == high
                pieces = []
                for c in range(3):
                    value = row(c)
                    top = value.astype(jnp.bfloat16).astype(jnp.float32)
                    pieces += [jnp.where(here, top, 0.0), jnp.where(here, value - top, 0.0)]
                lefts.append(jnp.concatenate(pieces, axis=0).astype(jnp.bfloat16))
                rights.append(
                    jnp.where(low_iota == where - high * float(LANES), 1.0, 0.0).astype(jnp.bfloat16)
                )
        left = jnp.concatenate(lefts, axis=1)
        right = jnp.concatenate(rights, axis=1)
        return total + lax.dot_general(left, right, NT, preferred_element_type=jnp.float32)

    total = lax.fori_loop(0, owners // 4, add, jnp.zeros((6 * high_rows, LANES), jnp.float32))
    for c in range(3):
        for h in range(halves):
            at = 2 * c * high_rows + h * tiles_dev
            out[c, :, h * LANES : (h + 1) * LANES] = (
                total[at : at + tiles_dev] + total[at + high_rows : at + high_rows + tiles_dev]
            )

    def sent(s, _):
        copy_to(s, *places).wait_send()
        copy_to(s, *amounts).wait_send()
        return 0

    lax.fori_loop(1, owners, sent, 0)


def per_device(
    nx, ny, photon_data, block_counts, gather_offsets, gather_blocks, albedo, gather_pixels, tile_slot
):
    cx, cy = photon_data.shape[1:3]
    points = gather_offsets.shape[1]
    steps = points // LANES
    owners = nx * ny
    tiles = tile_slot.shape[0]
    tiles_dev = tiles // owners
    cap_rows = -(-(3 * points // owners) // LANES)
    pitch = -(-3 * cap_rows // ROWS) * ROWS
    hb, vm = pl.BlockSpec(memory_space=pl.ANY), pl.BlockSpec(memory_space=pltpu.VMEM)
    dma, f32, i32, bf16 = pltpu.SemaphoreType.DMA, jnp.float32, jnp.int32, jnp.bfloat16
    stage_rows = LANES // ROWS * GROUP
    return pl.pallas_call(
        functools.partial(whole_kernel, nx, ny, cap_rows, tiles_dev),
        out_shape=jax.ShapeDtypeStruct((3, tiles_dev, TILE_PIX), f32),
        in_specs=[hb] * 7,
        out_specs=vm,
        scratch_shapes=[
            pltpu.VMEM((cx + 2, cy + 2, ROWS, LANES), f32),
            pltpu.VMEM((2, cy, ROWS, LANES), f32),
            pltpu.VMEM((2, cx, ROWS, LANES), f32),
            pltpu.VMEM((2, cx + 2, ROWS, LANES), f32),
            pltpu.VMEM((stage_rows, LANES), f32),
            pltpu.VMEM((stage_rows, LANES), f32),
            pltpu.VMEM((LANES, 3 * LANES), f32),
            pltpu.VMEM((LANES, 3 * LANES), f32),
            pltpu.VMEM((6 * owners, 2 * LANES), bf16),
            pltpu.VMEM((steps + 2, 3, LANES, LANES), f32),
            pltpu.VMEM((2, 3 * ROWS, 3 * LANES), bf16),
            pltpu.VMEM((LANES, LANES), bf16),
            pltpu.VMEM((cy, cx), i32),
            pltpu.VMEM((3, points), f32),
            pltpu.VMEM((4, points), i32),
            pltpu.VMEM((3, points), f32),
            pltpu.VMEM((steps, LANES), i32),
            pltpu.SMEM((tiles,), i32),
            pltpu.VMEM((cy, cx), f32),
            pltpu.VMEM((LANES, LANES), f32),
            pltpu.VMEM((ROWS, points), f32),
            pltpu.VMEM((2 * steps, LANES), i32),
            pltpu.SMEM((2 * steps, LANES), i32),
            pltpu.VMEM((steps + ROWS, LANES), i32),
            pltpu.VMEM((2 * owners, points), bf16),
            pltpu.VMEM((cap_rows * LANES, points), bf16),
            pltpu.VMEM((6 * owners, cap_rows * LANES), f32),
            pltpu.VMEM((owners, pitch, LANES), f32),
            pltpu.VMEM((owners, pitch, LANES), f32),
            pltpu.VMEM((owners, ROWS, LANES), f32),
            pltpu.VMEM((owners, ROWS, LANES), f32),
            dma((CHANNELS,)),
            dma((4 * CHANNELS,)),
            dma((6,)),
            dma,
            dma((8,)),
            dma((8,)),
            dma((owners,)),
            dma((owners,)),
            dma((owners,)),
            dma((owners,)),
        ],
        compiler_params=pltpu.CompilerParams(collective_id=0, has_side_effects=True),
        name="estimate",
    )(
        photon_data, block_counts.T, gather_offsets, gather_blocks, albedo,
        gather_pixels.reshape(steps, LANES), tile_slot,
    )


def solution(mesh):
    both = ("bx", "by")
    in_specs = (
        P(None, "bx", "by", None), P("bx", "by"), P(None, both), P(None, both),
        P(None, both), P(both), P(),
    )
    return jax.shard_map(
        functools.partial(per_device, mesh.shape["bx"], mesh.shape["by"]),
        mesh=mesh, in_specs=in_specs, out_specs=P(None, both, None), check_vma=False,
    )
```

```python
import functools

import jax
import jax.numpy as jnp
from jax import lax
from jax.experimental import pallas as pl
from jax.experimental.pallas import tpu as pltpu
from jax.sharding import PartitionSpec as P

TILE_PIX = 256
INV_RADIUS_SQ = 4.0
FAR = 1.0e4
LANES = 128
ROWS = 8
CHANNELS = 6
MESH = pl.DeviceIdType.MESH
NT = (((1,), (1,)), ((), ()))
PITCH = 9
GROUP = 2 * ROWS * PITCH


def split_by(value, size):
    if size & (size - 1) == 0:
        return value >> (size.bit_length() - 1), value & (size - 1)
    return lax.div(value, size), lax.rem(value, size)


def whole_kernel(
    nx, ny, cap_rows, tiles_dev,
    photons, counts_h, offsets_h, blocks_h, albedo_h, pixels_h, tile_slot_h, out,
    table, edge_x, edge_y, ring_y, stage_a, stage_b, wide_a, wide_b, side_v, partial,
    spread, tri, counts, offsets, blocks, albedo, pixels, tile_slot,
    count_row, count_col, points_v, base_v, base_s, owner_v, left_v, right_v,
    packed, send, recv, send_at, recv_at, high_v, low_v,
    fill_sem, edge_sem, small_sem, base_sem, halo_send, halo_recv, send_sem, recv_sem,
    at_send_sem, at_recv_sem,
):
    cx, cy = photons.shape[1], photons.shape[2]
    pitch_y = cy + 2
    grid_x, grid_y = cx * nx, cy * ny
    points = offsets.shape[1]
    steps = points // LANES
    owners = nx * ny
    pitch = send.shape[1]
    ix, iy = lax.axis_index("bx"), lax.axis_index("by")
    me = ix * ny + iy

    barrier = pltpu.get_barrier_semaphore()

    def peer(s):
        to = split_by(me + s, owners)[1]
        return to, split_by(to, ny)

    for s in range(1, owners):
        pl.semaphore_signal(barrier, inc=1, device_id=peer(s)[1], device_id_type=MESH)

    small = [
        pltpu.make_async_copy(src, dst, small_sem.at[n])
        for n, (src, dst) in enumerate(
            (
                (counts_h, counts), (blocks_h, blocks), (offsets_h, offsets),
                (pixels_h, pixels), (tile_slot_h, tile_slot), (albedo_h, albedo),
            )
        )
    ]
    edges = []
    for c in range(CHANNELS):
        for s, x in enumerate((cx - 1, 0)):
            edges.append(
                pltpu.make_async_copy(
                    photons.at[c, x], edge_x.at[s, :, c], edge_sem.at[len(edges)]
                )
            )
        for s, y in enumerate((cy - 1, 0)):
            edges.append(
                pltpu.make_async_copy(
                    photons.at[c, :, y], edge_y.at[s, :, c], edge_sem.at[len(edges)]
                )
            )
    fills = [
        pltpu.make_async_copy(
            photons.at[c], table.at[pl.ds(1, cx), pl.ds(1, cy), c], fill_sem.at[c]
        )
        for c in range(CHANNELS)
    ]
    small[0].start()
    for edge in edges:
        edge.start()
    for copy in small[1:]:
        copy.start()
    a = lax.broadcasted_iota(jnp.int32, (LANES, LANES), 0)
    b = lax.broadcasted_iota(jnp.int32, (LANES, LANES), 1)
    tri[...] = jnp.where(a < b, 1.0, 0.0).astype(jnp.bfloat16)
    for n, rows in enumerate(((0, 1, 2), (0, 3, 2))):
        a = lax.broadcasted_iota(jnp.int32, spread.shape[1:], 0) % ROWS
        b = lax.broadcasted_iota(jnp.int32, spread.shape[1:], 1) // LANES
        hit = (a == rows[0]) & (b == 0)
        for m in range(1, 3):
            hit = hit | ((a == rows[m]) & (b == m))
        spread[n] = jnp.where(hit, 1.0, 0.0).astype(jnp.bfloat16)
    packed[...] = jnp.zeros_like(packed)
    side_v[...] = jnp.zeros_like(side_v)
    points_v[...] = jnp.zeros_like(points_v)
    owner_v[...] = jnp.full(owner_v.shape, -1, jnp.int32)

    small[0].wait()
    count_row[...] = counts[...].astype(jnp.float32)
    square = jnp.concatenate(
        [count_row[...], jnp.zeros((cy, LANES - cx), jnp.float32)], axis=1
    )
    square = jnp.concatenate([square, jnp.zeros((LANES - cy, LANES), jnp.float32)], axis=0)
    count_col[...] = square.T
    lane = lax.broadcasted_iota(jnp.int32, (ROWS, LANES), 1).astype(jnp.float32)

    def hide(ref, first, column):
        rows = column.shape[0]
        for r in range(0, rows, ROWS):
            place = pl.ds(first + r * ROWS, ROWS, stride=ROWS)
            ref[place, :] = jnp.where(lane < column[r : r + ROWS], ref[place, :], FAR)

    for edge in edges:
        edge.wait()
    for fill in fills:
        fill.start()
    flat_x = edge_x.reshape(2 * cy * ROWS, LANES)
    flat_y = edge_y.reshape(2 * cx * ROWS, LANES)
    for s, y in enumerate((cy - 1, 0)):
        hide(flat_y, s * cx * ROWS, count_col[0:cx, y : y + 1])
    for s, x in enumerate((cx - 1, 0)):
        hide(flat_x, s * cy * ROWS, count_row[:, x : x + 1])
    pl.semaphore_wait(barrier, owners - 1)

    right, left = lax.rem(ix + 1, nx), lax.rem(ix + nx - 1, nx)
    up, down = lax.rem(iy + 1, ny), lax.rem(iy + ny - 1, ny)
    data = pl.ds(0, CHANNELS)
    wide_x, wide_y = pl.ds(1, cx), pl.ds(1, cy)
    parts = [
        (edge_y.at[0, :, data], ring_y.at[0, wide_x, data], ix, up),
        (edge_y.at[1, :, data], ring_y.at[1, wide_x, data], ix, down),
        (edge_x.at[0, :, data], table.at[0, wide_y, data], right, iy),
        (edge_x.at[1, :, data], table.at[cx + 1, wide_y, data], left, iy),
        (edge_x.at[0, cy - 1, data], ring_y.at[0, 0, data], right, up),
        (edge_x.at[0, 0, data], ring_y.at[1, 0, data], right, down),
        (edge_x.at[1, cy - 1, data], ring_y.at[0, cx + 1, data], left, up),
        (edge_x.at[1, 0, data], ring_y.at[1, cx + 1, data], left, down),
    ]
    halos = [
        pltpu.make_async_remote_copy(
            src_ref=src, dst_ref=dst, send_sem=halo_send.at[n], recv_sem=halo_recv.at[n],
            device_id=(px, py), device_id_type=MESH,
        )
        for n, (src, dst, px, py) in enumerate(parts)
    ]
    for halo in halos:
        halo.start()

    for copy in small[1:4]:
        copy.wait()
    cell_x, cell_y = split_by(blocks[...], grid_y)

    def local(cell, first, size):
        t = cell - first + 1
        t = jnp.where(t < 0, t + size, t)
        return jnp.where(t >= size, t - size, t)

    lx, ly = local(cell_x, ix * cx, grid_x), local(cell_y, iy * cy, grid_y)
    low_x, low_y = jnp.min(lx, axis=0, keepdims=True), jnp.min(ly, axis=0, keepdims=True)
    own_y = ly[0:1]
    other_y = 2 * low_y + 1 - own_y
    line = jnp.minimum(low_x, cx) * pitch_y
    bases = (
        line + jnp.clip(own_y, 0, cy + 1),
        line + jnp.clip(other_y, 0, cy + 1),
    )
    for n in range(2):
        for j in range(steps):
            base_v[n * steps + j : n * steps + j + 1, :] = bases[n][:, j * LANES : (j + 1) * LANES]
    to_scalar = pltpu.make_async_copy(base_v, base_s, base_sem)
    to_scalar.start()
    points_v[0:1, :] = offsets[0:1, :] + (lx[0:1] - low_x).astype(jnp.float32)
    points_v[1:2, :] = offsets[1:2, :]
    points_v[2:3, :] = offsets[2:3, :]
    points_v[3:4, :] = offsets[1:2, :] + (own_y - other_y).astype(jnp.float32)

    tile, within = split_by(pixels[...], TILE_PIX)
    small[4].wait()

    def look_up(t, found):
        for u in range(ROWS):
            n = t * ROWS + u
            found = jnp.where(tile == n, tile_slot[n], found)
        return found

    slot = lax.fori_loop(0, tile_slot.shape[0] // ROWS, look_up, jnp.zeros_like(tile))
    owner, place = split_by(slot, tiles_dev)
    half, low = split_by(within, LANES)
    first = half * tiles_dev + place
    owner_v[2 : 2 + steps, :] = owner

    own_iota = lax.broadcasted_iota(jnp.int32, (owners, LANES), 0)
    cap_iota = lax.broadcasted_iota(jnp.int32, (cap_rows * LANES, LANES), 0).astype(jnp.float32)
    carry = jnp.zeros((owners, LANES), jnp.float32)
    ones = jnp.ones((LANES, LANES), jnp.bfloat16)
    for j in range(steps):
        mine = own_iota == owner[j : j + 1, :]
        hot = jnp.where(mine, 1.0, 0.0).astype(jnp.bfloat16)
        before = jnp.dot(hot, tri[...], preferred_element_type=jnp.float32)
        rank = jnp.sum(jnp.where(mine, before + carry, 0.0), axis=0, keepdims=True)
        carry = carry + jnp.dot(hot, ones, preferred_element_type=jnp.float32)
        span = slice(j * LANES, (j + 1) * LANES)
        left_v[:, span] = jnp.concatenate(
            [
                jnp.where(mine, v[j : j + 1, :].astype(jnp.float32), 0.0).astype(jnp.bfloat16)
                for v in (first, low)
            ],
            axis=0,
        )
        right_v[:, span] = jnp.where(cap_iota == rank, 1.0, 0.0).astype(jnp.bfloat16)
    packed_at = lax.dot_general(left_v[...], right_v[...], NT, preferred_element_type=jnp.float32)
    packed_at = packed_at[:owners] * float(LANES) + packed_at[owners:]
    flat_at = send_at.reshape(owners * send_at.shape[1], LANES)
    for j in range(cap_rows):
        flat_at[pl.ds(j, owners, stride=send_at.shape[1]), :] = packed_at[
            :, j * LANES : (j + 1) * LANES
        ]

    for fill in fills:
        fill.wait()
    flat = table.reshape((cx + 2) * pitch_y * ROWS, LANES)
    cells = table.reshape((cx + 2) * pitch_y, ROWS, LANES)
    for x in range(cx):
        hide(flat, ((x + 1) * pitch_y + 1) * ROWS, count_row[:, x : x + 1])
    small[5].wait()
    to_scalar.wait()

    def widen(n, step, wide):
        value = points_v[:, pl.ds(pl.multiple_of(step * LANES, LANES), LANES)]
        pieces = []
        for _ in range(3):
            high = value.astype(jnp.bfloat16)
            pieces.append(high)
            value = value - high.astype(jnp.float32)
        wide[...] = lax.dot_general(
            jnp.concatenate(pieces, axis=0), spread[n], (((0,), (0,)), ((), ())),
            preferred_element_type=jnp.float32,
        )

    def load_group(n, step, g, stage):
        for p in range(ROWS):
            cell = base_s[n * steps + step, g * ROWS + p]
            for k in range(2):
                stage[pl.ds(g * GROUP + k * ROWS * PITCH + p, ROWS, stride=PITCH), :] = cells[
                    cell + k * pitch_y
                ]

    def sum_group(g, stage, wide, totals):
        here = slice(g * ROWS, g * ROWS + ROWS)
        x0, y0, z0 = (wide[here, n * LANES : (n + 1) * LANES] for n in range(3))
        for k, x in enumerate((x0, x0 - 1.0)):
            def chan(c):
                return stage[pl.ds(g * GROUP + (k * ROWS + c) * PITCH, ROWS), :]

            ex, ey, ez = chan(0) - x, chan(1) - y0, chan(2) - z0
            d2 = ex * ex + ey * ey + ez * ez
            w = jnp.maximum(1.0 - d2 * INV_RADIUS_SQ, 0.0)
            for c in range(3):
                term = w * chan(3 + c)
                totals[c] = term if totals[c] is None else totals[c] + term
        return totals

    def first_half(now, later, stages, wides):
        widen(0, later, wides[1])
        for g in range(LANES // ROWS):
            load_group(0, later, g, stages[1])
            totals = sum_group(g, stages[0], wides[0], [None] * 3)
            for c in range(3):
                partial[now + 2, c, g * ROWS : (g + 1) * ROWS, :] = totals[c]

    def first_two(i, _):
        n = 2 * i
        first_half(n, n + 1, (stage_a, stage_b), (wide_a, wide_b))
        first_half(n + 1, jnp.minimum(n + 2, steps - 1), (stage_b, stage_a), (wide_b, wide_a))
        return 0

    for halo in halos[2:4]:
        halo.wait()
    widen(0, 0, wide_a)
    for g in range(LANES // ROWS):
        load_group(0, 0, g, stage_a)
    lax.fori_loop(0, steps // 2, first_two, 0)

    for halo in halos[:2] + halos[4:]:
        halo.wait()
    for s, y in enumerate((0, cy + 1)):
        for x in range(cx + 2):
            table[x, y] = ring_y[s, x]

    def exchange(s, rows, source, target, send_at_sem, recv_at_sem):
        to, where = peer(s)
        return pltpu.make_async_remote_copy(
            src_ref=source.at[to, pl.ds(0, rows)],
            dst_ref=target.at[s, pl.ds(0, rows)],
            send_sem=send_at_sem,
            recv_sem=recv_at_sem,
            device_id=where,
            device_id_type=MESH,
        )

    def several(start, count, rows, target, send_at_sem, recv_at_sem):
        part = target.at[pl.ds(start, count), pl.ds(0, rows)]
        return pltpu.make_async_remote_copy(
            src_ref=part, dst_ref=part, send_sem=send_at_sem, recv_sem=recv_at_sem,
            device_id=peer(1)[1], device_id_type=MESH,
        )

    for s in range(1, owners):
        exchange(s, cap_rows, send_at, recv_at, at_send_sem, at_recv_sem).start()

    def pack(row, index, step):
        mine = own_iota == owner_v[pl.ds(row, 1), :]
        span = pl.ds(pl.multiple_of(step * LANES, LANES), LANES)
        pieces = []
        for c in range(3):
            rad = jnp.sum(partial[index, c].T, axis=0, keepdims=True) * albedo[c : c + 1, span]
            high = rad.astype(jnp.bfloat16).astype(jnp.float32)
            pieces += [high, rad - high]
        return jnp.concatenate(
            [jnp.where(mine, v, 0.0).astype(jnp.bfloat16) for v in pieces], axis=0
        )

    def second_half(now, later, stages, wides):
        widen(1, later, wides[1])
        for g in range(LANES // ROWS):
            load_group(1, later, g, stages[1])
            here = slice(g * ROWS, (g + 1) * ROWS)
            totals = sum_group(
                g, stages[0], wides[0], [partial[now + 2, c, here, :] for c in range(3)]
            )
            for c in range(3):
                partial[now + 2, c, here, :] = totals[c]

    def second_two(i, _):
        n = 2 * i
        span = pl.ds(pl.multiple_of(jnp.maximum(n - 4, 0) * LANES, LANES), 2 * LANES)
        packed[...] += lax.dot_general(
            side_v[...], right_v[:, span], NT, preferred_element_type=jnp.float32
        )
        for u in range(2):
            side_v[:, u * LANES : (u + 1) * LANES] = pack(n + u, n + u, jnp.maximum(n - 2, 0) + u)
        second_half(n, n + 1, (stage_a, stage_b), (wide_a, wide_b))
        second_half(n + 1, jnp.minimum(n + 2, steps - 1), (stage_b, stage_a), (wide_b, wide_a))
        return 0

    widen(1, 0, wide_a)
    for g in range(LANES // ROWS):
        load_group(1, 0, g, stage_a)
    lax.fori_loop(0, steps // 2, second_two, 0)
    sides = [side_v[...]] + [pack(steps + u, steps + u, steps - 2 + u) for u in range(2)]
    packed[...] += lax.dot_general(
        jnp.concatenate(sides, axis=1), right_v[:, (steps - 4) * LANES :], NT,
        preferred_element_type=jnp.float32,
    )

    flat_send = send.reshape(owners * pitch, LANES)

    def part(v, j):
        return packed[pl.ds(v * owners, owners), pl.ds(j * LANES, LANES)]

    for j in range(cap_rows):
        for c in range(3):
            flat_send[pl.ds(c * cap_rows + j, owners, stride=pitch), :] = (
                part(2 * c, j) + part(2 * c + 1, j)
            )

    for s in range(1, owners):
        exchange(s, 3 * cap_rows, send, recv, send_sem, recv_sem.at[s // 4]).start()
    recv[0] = send[me]
    recv_at[0] = send_at[me]
    everyone = several(1, owners - 1, cap_rows, recv_at, at_send_sem, at_recv_sem)
    everyone.wait_recv()

    halves = out.shape[2] // LANES
    high_rows = tiles_dev * halves
    high_iota = lax.broadcasted_iota(jnp.int32, (high_rows, LANES), 0).astype(jnp.float32)
    low_iota = lax.broadcasted_iota(jnp.int32, (LANES, LANES), 0).astype(jnp.float32)

    def spots(q, _):
        rights = []
        for u in range(4):
            blk = recv_at[q * 4 + u]
            for j in range(cap_rows):
                where = blk[j : j + 1]
                high = jnp.floor(where * (1.0 / LANES))
                at = (q * 4 + u) * ROWS + j
                high_v[pl.ds(at, 1), :] = high
                rights.append(
                    jnp.where(low_iota == where - high * float(LANES), 1.0, 0.0).astype(jnp.bfloat16)
                )
        low_v[q] = jnp.concatenate(rights, axis=1)
        return 0

    lax.fori_loop(0, owners // 4, spots, 0)

    def add(q, total):
        lefts = []
        for u in range(4):
            blk = recv[q * 4 + u]
            for j in range(cap_rows):
                here = high_iota == high_v[pl.ds((q * 4 + u) * ROWS + j, 1), :]
                pieces = []
                for c in range(3):
                    value = blk[c * cap_rows + j : c * cap_rows + j + 1]
                    top = value.astype(jnp.bfloat16).astype(jnp.float32)
                    pieces += [jnp.where(here, top, 0.0), jnp.where(here, value - top, 0.0)]
                lefts.append(jnp.concatenate(pieces, axis=0).astype(jnp.bfloat16))
        left = jnp.concatenate(lefts, axis=1)
        return total + lax.dot_general(left, low_v[q], NT, preferred_element_type=jnp.float32)

    def wait_add(q, total):
        several(q * 4, 4, 3 * cap_rows, recv, send_sem, recv_sem.at[q]).wait_recv()
        return add(q, total)

    several(1, 3, 3 * cap_rows, recv, send_sem, recv_sem.at[0]).wait_recv()
    total = add(0, jnp.zeros((6 * high_rows, LANES), jnp.float32))
    total = lax.fori_loop(1, owners // 4, wait_add, total)
    for c in range(3):
        for h in range(halves):
            at = 2 * c * high_rows + h * tiles_dev
            out[c, :, h * LANES : (h + 1) * LANES] = (
                total[at : at + tiles_dev] + total[at + high_rows : at + high_rows + tiles_dev]
            )

    everyone.wait_send()
    several(1, owners - 1, 3 * cap_rows, recv, send_sem, recv_sem.at[0]).wait_send()


def per_device(
    nx, ny, photon_data, block_counts, gather_offsets, gather_blocks, albedo, gather_pixels, tile_slot
):
    cx, cy = photon_data.shape[1:3]
    points = gather_offsets.shape[1]
    steps = points // LANES
    owners = nx * ny
    tiles = tile_slot.shape[0]
    tiles_dev = tiles // owners
    cap_rows = -(-(3 * points // owners) // LANES)
    pitch = -(-3 * cap_rows // ROWS) * ROWS
    hb, vm = pl.BlockSpec(memory_space=pl.ANY), pl.BlockSpec(memory_space=pltpu.VMEM)
    dma, f32, i32, bf16 = pltpu.SemaphoreType.DMA, jnp.float32, jnp.int32, jnp.bfloat16
    stage_rows = LANES // ROWS * GROUP
    return pl.pallas_call(
        functools.partial(whole_kernel, nx, ny, cap_rows, tiles_dev),
        out_shape=jax.ShapeDtypeStruct((3, tiles_dev, TILE_PIX), f32),
        in_specs=[hb] * 7,
        out_specs=vm,
        scratch_shapes=[
            pltpu.VMEM((cx + 2, cy + 2, ROWS, LANES), f32),
            pltpu.VMEM((2, cy, ROWS, LANES), f32),
            pltpu.VMEM((2, cx, ROWS, LANES), f32),
            pltpu.VMEM((2, cx + 2, ROWS, LANES), f32),
            pltpu.VMEM((stage_rows, LANES), f32),
            pltpu.VMEM((stage_rows, LANES), f32),
            pltpu.VMEM((LANES, 3 * LANES), f32),
            pltpu.VMEM((LANES, 3 * LANES), f32),
            pltpu.VMEM((6 * owners, 2 * LANES), bf16),
            pltpu.VMEM((steps + 2, 3, LANES, LANES), f32),
            pltpu.VMEM((2, 3 * ROWS, 3 * LANES), bf16),
            pltpu.VMEM((LANES, LANES), bf16),
            pltpu.VMEM((cy, cx), i32),
            pltpu.VMEM((3, points), f32),
            pltpu.VMEM((4, points), i32),
            pltpu.VMEM((3, points), f32),
            pltpu.VMEM((steps, LANES), i32),
            pltpu.SMEM((tiles,), i32),
            pltpu.VMEM((cy, cx), f32),
            pltpu.VMEM((LANES, LANES), f32),
            pltpu.VMEM((ROWS, points), f32),
            pltpu.VMEM((2 * steps, LANES), i32),
            pltpu.SMEM((2 * steps, LANES), i32),
            pltpu.VMEM((steps + ROWS, LANES), i32),
            pltpu.VMEM((2 * owners, points), bf16),
            pltpu.VMEM((cap_rows * LANES, points), bf16),
            pltpu.VMEM((6 * owners, cap_rows * LANES), f32),
            pltpu.VMEM((owners, pitch, LANES), f32),
            pltpu.VMEM((owners, pitch, LANES), f32),
            pltpu.VMEM((owners, ROWS, LANES), f32),
            pltpu.VMEM((owners, ROWS, LANES), f32),
            pltpu.VMEM((owners * ROWS, LANES), f32),
            pltpu.VMEM((owners // 4, LANES, 4 * cap_rows * LANES), bf16),
            dma((CHANNELS,)),
            dma((4 * CHANNELS,)),
            dma((6,)),
            dma,
            dma((8,)),
            dma((8,)),
            dma,
            dma((owners // 4,)),
            dma,
            dma,
        ],
        compiler_params=pltpu.CompilerParams(collective_id=0, has_side_effects=True),
        name="estimate",
    )(
        photon_data, block_counts.T, gather_offsets, gather_blocks, albedo,
        gather_pixels.reshape(steps, LANES), tile_slot,
    )


def solution(mesh):
    both = ("bx", "by")
    in_specs = (
        P(None, "bx", "by", None), P("bx", "by"), P(None, both), P(None, both),
        P(None, both), P(both), P(),
    )
    return jax.shard_map(
        functools.partial(per_device, mesh.shape["bx"], mesh.shape["by"]),
        mesh=mesh, in_specs=in_specs, out_specs=P(None, both, None), check_vma=False,
    )
```
